32 devices in a mesh: cand: 4 (over x, core), tp: 8 (over z, y).
Axes of the slice: x: 2, y: 2, z: 4, core: 2. Of those that a mesh axis runs over, the one named last changes fastest.
Arguments:
- start_state: float32 [128], replicated, may hold values from -6 to 6
- goal: float32 [128], replicated, may hold values from -6 to 6
- mean_prev: float32 [128], replicated, may hold values from -0.5 to 0.5
- std_prev: float32 [128], replicated, may hold values from 0.1 to 0.5
- noise: float32 [768, 128], P('cand'), may hold values from -23 to 23
- members: int32 [768, 1], P('cand'), may hold values from 0 to 3; in each aligned block of 192 rows (0 to 191, 192 to 383, ...) at most 60 rows name the same one
- elites: int32 [96], replicated, may hold values from 0 to 767, as said below
- w_in: bfloat16 [4, 144, 4096], P(None, None, 'tp'), may hold values from -0.5 to 0.5
- w_hid: bfloat16 [4, 4096, 4096], P(None, None, 'tp'), may hold values from -0.09375 to 0.09375
- w_out: bfloat16 [4, 4096, 128], P(None, 'tp'), may hold values from -0.09375 to 0.09375
Outputs:
- scores: float32 [768], P('cand')
- new_mean: float32 [128], replicated
- new_std: float32 [128], replicated
The draws below stay inside these ranges and needn't reach their ends.
Inputs may be any that keep to these rules, and one draw needn't show every extreme that they name: `members`: among the candidates of one index of cand no member is named more than 60 times. `elites`: 96 distinct candidate numbers.
All inputs are finite; a program needn't handle non-finite values.
Results may differ from the reference program's by a relative error of at most 0.0085.
Values may be sent and summed in bfloat16 or wider, within the bound.
A program may use at most 64 MiB of HBM per device.

```python
import math
import jax
import jax.numpy as jnp
import numpy as np
from jax import lax

H = 4096
S = 128
A = 16
HORIZON = 8
MEMBERS = 4
CAND_DEV = 192
CAP = 60
CANDS = 768
ELITES = 96
N_CAND = 4


def draw_noise(key, part):
    first_key, second_key = jax.random.split(key)
    position = jnp.arange(CANDS, dtype=jnp.float32) / max(CANDS - 1, 1)
    factor = jnp.exp(jax.random.uniform(second_key, (CANDS,), jnp.float32, math.log(0.5), math.log(1.5)))
    growth = jnp.exp(position * math.log(3.0))
    sample = jnp.clip(jax.random.normal(first_key, (CANDS, HORIZON * A), jnp.float32), -5.0, 5.0)
    return (sample * (growth * factor)[:, None]).astype(jnp.float32)


def draw_elites(key, part):
    return jax.random.permutation(jax.random.fold_in(key, 7), CANDS)[:ELITES].astype(jnp.int32)


def block_levels(own_key, dims, cuts, smallest, high):
    def one(dim, blocks):
        draws = jax.random.uniform(jax.random.fold_in(jax.random.fold_in(own_key, 6), dim), (blocks,), jnp.float32, smallest / len(cuts), high / len(cuts))
        return jnp.repeat(jnp.exp(draws), dims[dim] // blocks).reshape((-1,) + (1,) * (len(dims) - dim - 1))

    loudness = one(*cuts[0])
    for cut in cuts[1:]:
        loudness = loudness * one(*cut)
    return loudness


def shared_out(own_key, own, number, rows, amount, top, most, skew):
    ranking = jax.random.permutation(own_key, amount)
    packed, common = shares(amount, rows * top, most, skew, True), shares(amount, rows * top, most, skew, False)
    places = jnp.arange(amount)

    def named(sizes, turn):
        used = int((sizes > 0).sum())
        fixed = max(1, used // 4)
        passed = fixed + (places - fixed + turn * (used - fixed)) % max(1, amount - fixed)
        return jnp.zeros((amount,), jnp.int32).at[ranking[jnp.where(places < fixed, places, passed)]].set(jnp.asarray(sizes, jnp.int32))

    sizes = jnp.where(number % 4 == 0, named(packed, number // 4), named(common, number - number // 4 - 1))
    mixed = jax.random.permutation(jax.random.fold_in(own, 3), amount)
    source_of, receiver = mixed[0:amount // 2 * 2:2], mixed[1:amount // 2 * 2:2]
    slack = jnp.minimum(sizes[source_of] - 1, most - sizes[receiver]) // 2
    slack = jnp.where((source_of == ranking[0]) | (receiver == ranking[0]) | (sizes[receiver] == 0), 0, jnp.maximum(slack, 0))
    passed = jax.random.randint(jax.random.fold_in(own, 4), (amount // 2,), 0, 1 << 20) % (slack + 1)
    sizes = sizes.at[source_of].add(-passed).at[receiver].add(passed)
    items = jnp.searchsorted(jnp.cumsum(sizes), jnp.arange(rows * top), side="right").astype(jnp.int32)
    grid = items.reshape(top, rows).T
    grid = grid[jax.random.permutation(jax.random.fold_in(own, 1), rows)]
    turn = jax.random.randint(jax.random.fold_in(own, 2), (rows, 1), 0, top)
    return jnp.take_along_axis(grid, (jnp.arange(top)[None, :] + turn) % top, axis=1)


def shares(number_of, total, limit, slope, full):
    loads = [(1 << 20) // math.isqrt(standing ** slope) + 1 for standing in range(1, number_of + 1)]
    largest = limit if full else min(limit, max(-(-total // number_of), total * loads[0] // sum(loads)))
    least = 1 if total - largest >= number_of - 1 else 0
    given, surplus = [largest] + [least] * (number_of - 1), total - largest - least * (number_of - 1)
    while surplus > 0:
        free = [i for i in range(1, number_of) if given[i] < largest] or [i for i in range(1, number_of) if given[i] < limit]
        pool, left = sum([loads[i] for i in free]), surplus
        for i in free:
            addition = min(limit - given[i], max(1, left * loads[i] // pool), surplus)
            given[i] = given[i] + addition
            surplus = surplus - addition
    return np.array(given)


def normal_values(rng, shape, width, most, shards=(), kind=jnp.bfloat16):
    factor_of = block_levels(rng, shape, shards, -0.22, 0.18) if shards else 1.0
    drawn = jax.random.normal(rng, shape, jnp.float32) * width * factor_of
    return jnp.minimum(jnp.maximum(drawn, -most), most).astype(kind)


def setup_inputs(seed: int = 0) -> dict:
    splits = jax.random.split(jax.random.key(seed), 11)
    start_state = normal_values(splits[0], (S,), 1.0, 6.0, (), jnp.float32)
    goal = normal_values(splits[1], (S,), 1.0, 6.0, (), jnp.float32)
    mean_prev = jnp.clip(jax.random.uniform(splits[2], (HORIZON * A,), jnp.float32, -0.5, 0.5), -0.5, 0.5)
    std_prev = jnp.clip(jnp.exp(jax.random.uniform(splits[3], (HORIZON * A,), jnp.float32, math.log(0.1), math.log(0.5))), 0.1, 0.5)
    noise = draw_noise(jax.random.fold_in(splits[10], 71), 0)
    members_keys = jax.random.split(jax.random.fold_in(splits[5], 1), CANDS // CAND_DEV)
    members_turns = jax.random.permutation(jax.random.fold_in(splits[5], 3), CANDS // CAND_DEV)
    members = jax.vmap(lambda own, number: shared_out(jax.random.fold_in(splits[5], 2), own, number, CAND_DEV, MEMBERS, 1, CAP, 1))(members_keys, members_turns).reshape((CANDS, 1))
    elites = draw_elites(jax.random.fold_in(splits[10], 71), 0)
    w_in = normal_values(splits[7], (MEMBERS, S + A, H), (S + A) ** -0.5, 0.5, ((2, 8),))
    w_hid = normal_values(splits[8], (MEMBERS, H, H), H ** -0.5, 0.09375, ((2, 8),))
    w_out = normal_values(splits[9], (MEMBERS, H, S), H ** -0.5, 0.09375, ((1, 8),))
    return {"start_state": start_state, "goal": goal, "mean_prev": mean_prev, "std_prev": std_prev, "noise": noise, "members": members, "elites": elites, "w_in": w_in, "w_hid": w_hid, "w_out": w_out}


def slot_matrix(member_block, member_count, capacity):
    onehot = (member_block[:, 0:1] == jnp.arange(member_count, dtype=jnp.int32)[None, :]).astype(jnp.float32)
    before = jnp.cumsum(onehot, axis=0) - onehot
    position = lax.optimization_barrier(jnp.sum(before * onehot, axis=1)).astype(jnp.int32)
    slot_number = member_block[:, 0].astype(jnp.int32) * capacity + position
    return (slot_number[None, :] == jnp.arange(member_count * capacity, dtype=jnp.int32)[:, None]).astype(jnp.float32)

def reward_of(states, goal, action):
    return -lax.optimization_barrier(jnp.mean((states - goal[None, :]) ** 2, axis=1)) - 0.1 * lax.optimization_barrier(jnp.mean(action * action, axis=1))

def reference(start_state, goal, mean_prev, std_prev, noise, members, elites, w_in, w_hid, w_out):
    actions = mean_prev[None, :] + std_prev[None, :] * noise

    def one_block(pair):
        block_actions, block_members = pair
        dispatch = slot_matrix(block_members, MEMBERS, CAP)
        slot_actions = jnp.dot(dispatch, block_actions, precision=lax.Precision.HIGHEST)
        slot_actions = slot_actions.reshape(MEMBERS, CAP, HORIZON, A)
        gathered = []
        for member in range(MEMBERS):
            states = jnp.zeros((CAP, S), jnp.float32) + start_state[None, :]
            running = jnp.zeros((CAP,), jnp.float32)
            for step_index in range(HORIZON):
                action = slot_actions[member, :, step_index, :]
                inputs = jnp.concatenate([states, action], axis=1).astype(jnp.bfloat16)
                hidden_one = jax.nn.silu(jnp.dot(inputs, w_in[member], preferred_element_type=jnp.float32)).astype(jnp.bfloat16)
                hidden_two = jax.nn.silu(jnp.dot(hidden_one, w_hid[member], preferred_element_type=jnp.float32)).astype(jnp.bfloat16)
                change = jnp.dot(hidden_two, w_out[member], preferred_element_type=jnp.float32)
                states = states + change
                running = running + reward_of(states, goal, action)
            gathered.append(running)
        slot_returns = jnp.concatenate(gathered)
        return jnp.dot(slot_returns, dispatch, precision=lax.Precision.HIGHEST)
    returns = lax.map(one_block, (actions.reshape(N_CAND, CAND_DEV, HORIZON * A), members.reshape(N_CAND, CAND_DEV, 1)))
    returns = returns.reshape(CANDS)
    return_mean = jnp.sum(returns) / CANDS
    return_var = jnp.sum((returns - return_mean) ** 2) / CANDS
    scores = (returns - return_mean) / jnp.sqrt(return_var + 1e-06)
    chosen = jnp.zeros((CANDS,), jnp.float32).at[elites].set(1.0)
    weights = chosen * (0.5 + jax.nn.sigmoid(scores))
    weight_sum = jnp.sum(weights)
    new_mean = jnp.dot(weights, actions, precision=lax.Precision.HIGHEST) / weight_sum
    new_var = jnp.dot(weights, (actions - new_mean[None, :]) ** 2, precision=lax.Precision.HIGHEST) / weight_sum
    new_std = jnp.sqrt(new_var + 1e-06)
    return (scores, new_mean, new_std)
```

```python
import functools
import jax
import jax.numpy as jnp
from jax import lax
from jax.experimental import pallas as pl
from jax.experimental.pallas import tpu as pltpu
from jax.sharding import PartitionSpec as P

HORIZON = 8
F32 = jnp.float32
BF16 = jnp.bfloat16
HI = lax.Precision.HIGHEST


def silu(v):
    h = 0.5 * v
    return h + h * jnp.tanh(h)


def kernel(
    n_cand, n_tp, cap,
    start_ref, goal_ref, mean_ref, std_ref, noise_ref, members_ref, elites_ref,
    win_hbm, whid_hbm, wout_hbm,
    scores_ref, new_mean_ref, new_std_ref,
    win_v, whid_v, wout_v, h1_v, pf, ps, rs_rx, xs, xs_send, state, sq, big,
    act_send, act_rx, act_t, sa_all, meta_all, ret_all,
    load_sem, win_s, win_r, act_s, act_r, sa_s, sa_r, meta_s, meta_r,
    rs_s, rs_r, ag_s, ag_r, ret_s, ret_r,
):
    n_mem = win_hbm.shape[0]
    chunk = win_hbm.shape[2]
    width = start_ref.shape[1]
    local = noise_ref.shape[0]
    rows = n_mem * cap
    own = rows // n_tp
    a_dim = mean_ref.shape[1] // HORIZON
    c = lax.axis_index("cand")
    t = lax.axis_index("tp")
    m = lax.rem(c, n_mem)
    group = c - m

    def tp_peer(d):
        return lax.rem(t + d, n_tp)

    def remote(src, dst, s, r, cc, tt):
        return pltpu.make_async_remote_copy(
            src_ref=src, dst_ref=dst, send_sem=s, recv_sem=r,
            device_id={"cand": cc, "tp": tt}, device_id_type=pl.DeviceIdType.MESH,
        )

    win_copies = [
        remote(win_hbm.at[m], win_v.at[d], win_s.at[d], win_r.at[d], c, tp_peer(d))
        for d in range(1, n_tp)
    ]
    for cp in win_copies:
        cp.start()
    loads = [pltpu.make_async_copy(win_hbm.at[m], win_v.at[0], load_sem.at[n_tp])]
    for d in range(n_tp):
        src = lax.rem(t + n_tp - d, n_tp)
        loads.append(pltpu.make_async_copy(
            whid_hbm.at[m, pl.ds(pl.multiple_of(src * chunk, chunk), chunk), :],
            whid_v.at[pl.ds(d * chunk, chunk), :], load_sem.at[d]))
    loads.append(pltpu.make_async_copy(wout_hbm.at[m], wout_v, load_sem.at[n_tp + 1]))
    for cp in loads:
        cp.start()

    actions = mean_ref[...] + std_ref[...] * noise_ref[...]
    members = members_ref[...]
    lane = lax.broadcasted_iota(jnp.int32, (local, 128), 1)
    onehot = (members == lane).astype(F32)
    lower = (
        lax.broadcasted_iota(jnp.int32, (local, local), 1)
        < lax.broadcasted_iota(jnp.int32, (local, local), 0)
    ).astype(BF16)
    before = jnp.dot(lower, onehot.astype(BF16), preferred_element_type=F32)
    position = jnp.sum(before * onehot, axis=1, keepdims=True).astype(jnp.int32)
    slot = members * cap + position
    place = slot == lax.broadcasted_iota(jnp.int32, (local, rows), 1)
    place_f = place.astype(F32)
    over_cands = (((0,), (0,)), ((), ()))
    act_send[...] = lax.dot_general(
        place_f.astype(BF16), actions.astype(BF16), over_cands, preferred_element_type=F32
    ).astype(BF16)
    mine = pl.multiple_of(m * cap, cap)
    act_copies = []
    for k in range(1, n_mem):
        m2 = lax.rem(m + k, n_mem)
        act_copies.append(remote(
            act_send.at[pl.ds(pl.multiple_of(m2 * cap, cap), cap), :],
            act_rx.at[pl.ds(mine, cap), :], act_s.at[k], act_r.at[k], group + m2, t))
    for cp in act_copies:
        cp.start()
    act_rx[pl.ds(mine, cap), :] = act_send[pl.ds(mine, cap), :]

    numbers = c * local + lax.broadcasted_iota(jnp.int32, (local, 1), 0)
    chosen = jnp.sum((numbers == elites_ref[...]).astype(F32), axis=1, keepdims=True)
    action_cost = jnp.sum(actions * actions, axis=1, keepdims=True) * (0.1 / a_dim)
    facts = jnp.where(lane == 0, 1.0, jnp.where(lane == 1, chosen, jnp.where(lane == 2, action_cost, 0.0)))
    sa_all[c] = lax.dot_general(place_f, actions, over_cands, precision=HI, preferred_element_type=F32)
    meta_all[c] = lax.dot_general(facts, place_f, over_cands, precision=HI, preferred_element_type=F32)[:8]
    side_copies = []
    for k in range(1, n_cand):
        c2 = lax.rem(c + k, n_cand)
        side_copies.append(remote(meta_all.at[c], meta_all.at[c], meta_s.at[k], meta_r.at[k], c2, t))
        side_copies.append(remote(sa_all.at[c], sa_all.at[c], sa_s.at[k], sa_r.at[k], c2, t))
    for cp in side_copies:
        cp.start()

    state[...] = jnp.broadcast_to(start_ref[...], state.shape)
    sq[...] = jnp.zeros_like(sq)
    xs[...] = jnp.broadcast_to(start_ref[...], xs.shape).astype(BF16)
    for cp in act_copies:
        cp.wait_recv()
    for s in range(HORIZON):
        act_t[s] = act_rx[...].astype(F32)[:, s * a_dim:(s + 1) * a_dim].astype(BF16)
    for cp in loads:
        cp.wait()
    for cp in win_copies:
        cp.wait_recv()

    half = min(256, chunk)
    first_own = pl.multiple_of(t * own, own)

    def step_body(step, carry):
        x = jnp.concatenate([xs[...], act_t[step]], axis=1)
        for d in range(n_tp):
            h1_v[:, d * chunk:(d + 1) * chunk] = silu(
                jnp.dot(x, win_v[d], preferred_element_type=F32)).astype(BF16)
        total = None
        for n in range(chunk // half):
            h2 = silu(jnp.dot(h1_v[...], whid_v[:, n * half:(n + 1) * half],
                              preferred_element_type=F32)).astype(BF16)
            part = jnp.dot(h2, wout_v[n * half:(n + 1) * half, :], preferred_element_type=F32)
            total = part if total is None else total + part
        pf[...] = total
        ps[...] = total.astype(BF16)
        rs = [
            remote(ps.at[pl.ds(pl.multiple_of(tp_peer(d) * own, own), own), :], rs_rx.at[d],
                   rs_s.at[d], rs_r.at[d], c, tp_peer(d))
            for d in range(1, n_tp)
        ]
        for cp in rs:
            cp.start()
        change = pf[pl.ds(first_own, own), :]
        for d in range(1, n_tp):
            rs[d - 1].wait_recv()
            change = change + rs_rx[d].astype(F32)
        new_state = state[...] + change
        state[...] = new_state
        ag = [
            remote(xs_send, xs.at[pl.ds(first_own, own), :], ag_s.at[d], ag_r.at[d], c, tp_peer(d))
            for d in range(1, n_tp)
        ]

        @pl.when(step < HORIZON - 1)
        def _():
            xs_send[...] = new_state.astype(BF16)
            for cp in ag:
                cp.start()
            xs[pl.ds(first_own, own), :] = new_state.astype(BF16)

        gap = new_state - goal_ref[...]
        sq[...] += gap * gap
        for cp in rs:
            cp.wait_send()

        @pl.when(step < HORIZON - 1)
        def _():
            for cp in ag:
                cp.wait()

        return carry

    lax.fori_loop(0, HORIZON, step_body, 0)

    big[...] = jnp.zeros_like(big)
    big[pl.ds(pl.multiple_of(m * cap + lax.rem(t * own, cap), own), own), :] = sq[...] * (1.0 / width)
    row = lax.dot_general(jnp.ones((8, width), F32), big[...], (((1,), (1,)), ((), ())),
                          precision=HI, preferred_element_type=F32)
    me = c * n_tp + t
    ret_all[me] = row[0:1]
    ret_copies = []
    for kc in range(n_cand):
        for kt in range(n_tp):
            if kc + kt:
                i = kc * n_tp + kt
                ret_copies.append(remote(ret_all.at[me], ret_all.at[me], ret_s.at[i], ret_r.at[i],
                                         lax.rem(c + kc, n_cand), tp_peer(kt)))
    for cp in ret_copies:
        cp.start()
    for cp in side_copies:
        cp.wait_recv()
    for cp in ret_copies:
        cp.wait_recv()

    per_block = cap // own
    returns = []
    for b in range(n_cand):
        parts = [ret_all[(b - b % n_mem + m2) * n_tp + b % n_mem * per_block + h]
                 for m2 in range(n_mem) for h in range(per_block)]
        returns.append(-functools.reduce(jnp.add, parts) - meta_all[b, 2:3, :])
    count = local * n_cand

    def over(vals):
        return jnp.sum(functools.reduce(jnp.add, vals), axis=1, keepdims=True)

    valid = [meta_all[b, 0:1, :] for b in range(n_cand)]
    mean = over([valid[b] * returns[b] for b in range(n_cand)]) / count
    var = over([valid[b] * (returns[b] - mean) ** 2 for b in range(n_cand)]) / count
    scale = jnp.sqrt(var + 1e-06)
    scores = [(returns[b] - mean) / scale for b in range(n_cand)]
    weights = [meta_all[b, 1:2, :] * (0.5 + 1.0 / (1.0 + jnp.exp(-scores[b]))) for b in range(n_cand)]
    weight_sum = over(weights)

    def moment(values):
        rows8 = [jnp.broadcast_to(weights[b], (8, rows)) for b in range(n_cand)]
        return functools.reduce(jnp.add, [
            jnp.dot(rows8[b], values(b), precision=HI, preferred_element_type=F32)
            for b in range(n_cand)])[0:1] / weight_sum

    new_mean = moment(lambda b: sa_all[b])
    new_mean_ref[...] = new_mean
    new_std_ref[...] = jnp.sqrt(moment(lambda b: (sa_all[b] - new_mean) ** 2) + 1e-06)

    my_parts = [ret_all[(group + m2) * n_tp + m * per_block + h]
                for m2 in range(n_mem) for h in range(per_block)]
    my_returns = -functools.reduce(jnp.add, my_parts) - meta_all[c, 2:3, :]
    my_scores = jnp.broadcast_to((my_returns - mean) / scale, (8, rows))
    scores_ref[...] = lax.dot_general(my_scores, place_f, (((1,), (1,)), ((), ())),
                                      precision=HI, preferred_element_type=F32)[0:1]

    for cp in win_copies + act_copies + side_copies + ret_copies:
        cp.wait_send()


def on_device(n_cand, n_tp, start_state, goal, mean_prev, std_prev, noise, members, elites, w_in, w_hid, w_out):
    local = noise.shape[0]
    n_mem, depth, chunk = w_in.shape
    width = start_state.shape[0]
    flat = mean_prev.shape[0]
    hidden = w_hid.shape[1]
    cap = -(-(5 * local // 16) // 16) * 16
    rows = n_mem * cap
    own = rows // n_tp
    total = n_cand * n_tp
    vmem = pl.BlockSpec(memory_space=pltpu.VMEM)
    hbm = pl.BlockSpec(memory_space=pl.ANY)
    dma = pltpu.SemaphoreType.DMA
    scores, new_mean, new_std = pl.pallas_call(
        functools.partial(kernel, n_cand, n_tp, cap),
        out_shape=(
            jax.ShapeDtypeStruct((1, local), F32),
            jax.ShapeDtypeStruct((1, flat), F32),
            jax.ShapeDtypeStruct((1, flat), F32),
        ),
        in_specs=[vmem] * 7 + [hbm] * 3,
        out_specs=(vmem,) * 3,
        scratch_shapes=[
            pltpu.VMEM((n_tp, depth, chunk), BF16),
            pltpu.VMEM((hidden, chunk), BF16),
            pltpu.VMEM((chunk, width), BF16),
            pltpu.VMEM((rows, hidden), BF16),
            pltpu.VMEM((rows, width), F32),
            pltpu.VMEM((rows, width), BF16),
            pltpu.VMEM((n_tp, own, width), BF16),
            pltpu.VMEM((rows, width), BF16),
            pltpu.VMEM((own, width), BF16),
            pltpu.VMEM((own, width), F32),
            pltpu.VMEM((own, width), F32),
            pltpu.VMEM((rows, width), F32),
            pltpu.VMEM((rows, flat), BF16),
            pltpu.VMEM((rows, flat), BF16),
            pltpu.VMEM((HORIZON, rows, flat // HORIZON), BF16),
            pltpu.VMEM((n_cand, rows, flat), F32),
            pltpu.VMEM((n_cand, 8, rows), F32),
            pltpu.VMEM((total, 1, rows), F32),
            dma((n_tp + 2,)),
            dma((n_tp,)), dma((n_tp,)),
            dma((n_mem,)), dma((n_mem,)),
            dma((n_cand,)), dma((n_cand,)),
            dma((n_cand,)), dma((n_cand,)),
            dma((n_tp,)), dma((n_tp,)),
            dma((n_tp,)), dma((n_tp,)),
            dma((total,)), dma((total,)),
        ],
        compiler_params=pltpu.CompilerParams(has_side_effects=True, vmem_limit_bytes=56 << 20),
    )(
        start_state.reshape(1, -1), goal.reshape(1, -1), mean_prev.reshape(1, -1),
        std_prev.reshape(1, -1), noise, members, elites.reshape(1, -1), w_in, w_hid, w_out,
    )
    return scores.reshape(-1), new_mean.reshape(-1), new_std.reshape(-1)


def solution(mesh):
    placed = (
        P(), P(), P(), P(), P("cand", None), P("cand", None), P(),
        P(None, None, "tp"), P(None, None, "tp"), P(None, "tp", None),
    )
    return jax.shard_map(
        functools.partial(on_device, mesh.shape["cand"], mesh.shape["tp"]),
        mesh=mesh, in_specs=placed, out_specs=(P("cand"), P(), P()), check_vma=False,
    )
```

```python
import functools
import jax
import jax.numpy as jnp
from jax import lax
from jax.experimental import pallas as pl
from jax.experimental.pallas import tpu as pltpu
from jax.sharding import PartitionSpec as P

HORIZON = 8
F32 = jnp.float32
BF16 = jnp.bfloat16
HI = lax.Precision.HIGHEST


def silu(v):
    h = 0.5 * v
    return h + h * jnp.tanh(h)


def kernel(
    n_cand, n_tp, cap,
    start_ref, goal_ref, mean_ref, std_ref, noise_ref, members_ref, elites_ref,
    win_hbm, whid_hbm, wout_hbm,
    scores_ref, new_mean_ref, new_std_ref,
    win_v, whid_v, wout_v, h1_v, pf, ps, rs_rx, xs, xs_send, state, sq, big,
    act_send, act_rx, act_t, sa_all, meta_all, ret_all,
    load_sem, win_s, win_r, act_s, act_r, sa_s, sa_r, meta_s, meta_r,
    rs_s, rs_r, ag_s, ag_r, ret_s, ret_r,
):
    n_mem = win_hbm.shape[0]
    chunk = win_hbm.shape[2]
    width = start_ref.shape[1]
    local = noise_ref.shape[0]
    rows = n_mem * cap
    lowest = n_tp // 4
    owners = range(lowest, n_tp - lowest)
    n_own = len(owners)
    own = rows // n_own
    a_dim = mean_ref.shape[1] // HORIZON
    c = lax.axis_index("cand")
    t = lax.axis_index("tp")
    m = lax.rem(c, n_mem)
    group = c - m

    def tp_peer(d):
        return lax.rem(t + d, n_tp)

    def remote(src, dst, s, r, cc, tt):
        return pltpu.make_async_remote_copy(
            src_ref=src, dst_ref=dst, send_sem=s, recv_sem=r,
            device_id={"cand": cc, "tp": tt}, device_id_type=pl.DeviceIdType.MESH,
        )

    pair = t + 1 - 2 * lax.rem(t, 2)
    win_copies = [
        remote(win_hbm.at[m], win_v.at[t], win_s.at[d], win_r.at[t], c, pair if d == 1 else tp_peer(d))
        for d in [1] + list(range(2, n_tp, 2))
    ]
    for cp in win_copies:
        cp.start()

    def arrived(d):
        src = lax.rem(t + n_tp - d, n_tp)
        return remote(win_hbm.at[m], win_v.at[src], win_s.at[0], win_r.at[src], c, pair)

    loads = [
        pltpu.make_async_copy(win_hbm.at[m], win_v.at[t], load_sem.at[0]),
        pltpu.make_async_copy(whid_hbm.at[m], whid_v, load_sem.at[1]),
    ]
    loads.append(pltpu.make_async_copy(wout_hbm.at[m], wout_v, load_sem.at[2]))
    for cp in loads:
        cp.start()

    actions = mean_ref[...] + std_ref[...] * noise_ref[...]
    members = members_ref[...]
    lane = lax.broadcasted_iota(jnp.int32, (local, 128), 1)
    onehot = (members == lane).astype(F32)
    lower = (
        lax.broadcasted_iota(jnp.int32, (local, local), 1)
        < lax.broadcasted_iota(jnp.int32, (local, local), 0)
    ).astype(BF16)
    before = jnp.dot(lower, onehot.astype(BF16), preferred_element_type=F32)
    position = jnp.sum(before * onehot, axis=1, keepdims=True).astype(jnp.int32)
    slot = members * cap + position
    place = slot == lax.broadcasted_iota(jnp.int32, (local, rows), 1)
    place_f = place.astype(F32)
    over_cands = (((0,), (0,)), ((), ()))
    act_send[...] = lax.dot_general(
        place_f.astype(BF16), actions.astype(BF16), over_cands, preferred_element_type=F32
    ).astype(BF16)
    mine = pl.multiple_of(m * cap, cap)
    act_copies = []
    for k in range(1, n_mem):
        m2 = lax.rem(m + k, n_mem)
        act_copies.append(remote(
            act_send.at[pl.ds(pl.multiple_of(m2 * cap, cap), cap), :],
            act_rx.at[pl.ds(mine, cap), :], act_s.at[k], act_r.at[k], group + m2, t))
    for cp in act_copies:
        cp.start()
    act_rx[pl.ds(mine, cap), :] = act_send[pl.ds(mine, cap), :]

    numbers = c * local + lax.broadcasted_iota(jnp.int32, (local, 1), 0)
    chosen = jnp.sum((numbers == elites_ref[...]).astype(F32), axis=1, keepdims=True)
    action_cost = jnp.sum(actions * actions, axis=1, keepdims=True) * (0.1 / a_dim)
    facts = jnp.where(lane == 0, 1.0, jnp.where(lane == 1, chosen, jnp.where(lane == 2, action_cost, 0.0)))
    sa_all[c] = lax.dot_general(place_f, actions, over_cands, precision=HI, preferred_element_type=F32)
    meta_all[c] = lax.dot_general(facts, place_f, over_cands, precision=HI, preferred_element_type=F32)[:8]
    side_copies = []
    for k in range(1, n_cand):
        c2 = lax.rem(c + k, n_cand)
        side_copies.append(remote(meta_all.at[c], meta_all.at[c], meta_s.at[k], meta_r.at[k], c2, t))
        side_copies.append(remote(sa_all.at[c], sa_all.at[c], sa_s.at[k], sa_r.at[k], c2, t))
    for cp in side_copies:
        cp.start()

    state[...] = jnp.broadcast_to(start_ref[...], state.shape)
    sq[...] = jnp.zeros_like(sq)
    xs[...] = jnp.broadcast_to(start_ref[...], xs.shape).astype(BF16)
    for cp in act_copies:
        cp.wait_recv()
    for s in range(HORIZON):
        act_t[s] = act_rx[...].astype(F32)[:, s * a_dim:(s + 1) * a_dim].astype(BF16)
    for cp in loads:
        cp.wait()
    for d in range(2, n_tp, 2):
        arrived(d).wait_recv()
        src = lax.rem(t + n_tp - d, n_tp)
        cp = remote(win_v.at[src], win_v.at[src], win_s.at[d + 1], win_r.at[src], c, pair)
        cp.start()
        win_copies.append(cp)
    for d in range(1, n_tp, 2):
        arrived(d).wait_recv()

    half = min(256, chunk)
    owner = jnp.logical_and(t >= owners[0], t <= owners[-1])
    place_own = t - lowest
    first_own = pl.multiple_of(place_own * own, own)

    def step_body(step, carry):
        rs = [
            remote(ps.at[pl.ds(i * own, own), :], rs_rx.at[t], rs_s.at[i], rs_r.at[t], c, o)
            for i, o in enumerate(owners)
        ]
        for q in range(2):
            lo, hi = q * rows // 2, (q + 1) * rows // 2
            held = range(q * n_own // 2, (q + 1) * n_own // 2)

            @pl.when(step > 0)
            def _():
                for i in held:
                    pl.when(t != owners[i])(remote(
                        xs_send, xs.at[pl.ds(i * own, own), :], ag_s.at[0], ag_r.at[i], c, pair).wait_recv)

            x = jnp.concatenate([xs[lo:hi, :], act_t[step, lo:hi, :]], axis=1)
            for d in range(n_tp):
                h1_v[lo:hi, d * chunk:(d + 1) * chunk] = silu(
                    jnp.dot(x, win_v[d], preferred_element_type=F32)).astype(BF16)
            total = None
            for n in range(chunk // half):
                h2 = silu(jnp.dot(h1_v[lo:hi, :], whid_v[:, n * half:(n + 1) * half],
                                  preferred_element_type=F32)).astype(BF16)
                part = jnp.dot(h2, wout_v[n * half:(n + 1) * half, :], preferred_element_type=F32)
                total = part if total is None else total + part
            pf[lo:hi, :] = total
            ps[lo:hi, :] = total.astype(BF16)
            for i in held:
                pl.when(t != owners[i])(rs[i].start)

        @pl.when(owner)
        def _():
            change = pf[pl.ds(first_own, own), :]
            for d in range(1, n_tp):
                src = lax.rem(t + n_tp - d, n_tp)
                remote(ps.at[pl.ds(0, own), :], rs_rx.at[src], rs_s.at[0], rs_r.at[src], c, pair).wait_recv()
                change = change + rs_rx[src].astype(F32)
            new_state = state[...] + change
            state[...] = new_state

            ag = [
                remote(xs_send, xs.at[pl.ds(first_own, own), :], ag_s.at[d], ag_r.at[place_own], c, tp_peer(d))
                for d in range(1, n_tp)
            ]

            @pl.when(step < HORIZON - 1)
            def _():
                xs_send[...] = new_state.astype(BF16)
                for cp in ag:
                    cp.start()
                xs[pl.ds(first_own, own), :] = new_state.astype(BF16)

            gap = new_state - goal_ref[...]
            sq[...] += gap * gap

            @pl.when(step < HORIZON - 1)
            def _():
                for cp in ag:
                    cp.wait_send()

        for o, cp in zip(owners, rs):
            pl.when(t != o)(cp.wait_send)

        return carry

    lax.fori_loop(0, HORIZON, step_body, 0)

    me = c * n_own + place_own
    ret_copies = [
        remote(ret_all.at[me], ret_all.at[me], ret_s.at[kc * n_tp + kt], ret_r.at[me],
               lax.rem(c + kc, n_cand), tp_peer(kt))
        for kc in range(n_cand) for kt in range(n_tp) if kc + kt
    ]

    @pl.when(owner)
    def _():
        big[...] = jnp.zeros_like(big)
        big[pl.ds(pl.multiple_of(m * cap + lax.rem(first_own, cap), own), own), :] = sq[...] * (1.0 / width)
        row = lax.dot_general(jnp.ones((8, width), F32), big[...], (((1,), (1,)), ((), ())),
                              precision=HI, preferred_element_type=F32)
        ret_all[me] = row[0:1]
        for cp in ret_copies:
            cp.start()

    for cp in side_copies:
        cp.wait_recv()
    for cc in range(n_cand):
        for i, o in enumerate(owners):
            k = cc * n_own + i
            pl.when(jnp.logical_or(t != o, c != cc))(remote(
                ret_all.at[k], ret_all.at[k], ret_s.at[0], ret_r.at[k], c, pair).wait_recv)

    per_block = cap // own
    returns = []
    for b in range(n_cand):
        parts = [ret_all[(b - b % n_mem + m2) * n_own + b % n_mem * per_block + h]
                 for m2 in range(n_mem) for h in range(per_block)]
        returns.append(-functools.reduce(jnp.add, parts) - meta_all[b, 2:3, :])
    count = local * n_cand

    def over(vals):
        return jnp.sum(functools.reduce(jnp.add, vals), axis=1, keepdims=True)

    valid = [meta_all[b, 0:1, :] for b in range(n_cand)]
    mean = over([valid[b] * returns[b] for b in range(n_cand)]) / count
    var = over([valid[b] * (returns[b] - mean) ** 2 for b in range(n_cand)]) / count
    scale = jnp.sqrt(var + 1e-06)
    scores = [(returns[b] - mean) / scale for b in range(n_cand)]
    weights = [meta_all[b, 1:2, :] * (0.5 + 1.0 / (1.0 + jnp.exp(-scores[b]))) for b in range(n_cand)]
    weight_sum = over(weights)

    def moment(values):
        rows8 = [jnp.broadcast_to(weights[b], (8, rows)) for b in range(n_cand)]
        return functools.reduce(jnp.add, [
            jnp.dot(rows8[b], values(b), precision=HI, preferred_element_type=F32)
            for b in range(n_cand)])[0:1] / weight_sum

    new_mean = moment(lambda b: sa_all[b])
    new_mean_ref[...] = new_mean
    new_std_ref[...] = jnp.sqrt(moment(lambda b: (sa_all[b] - new_mean) ** 2) + 1e-06)

    my_parts = [ret_all[(group + m2) * n_own + m * per_block + h]
                for m2 in range(n_mem) for h in range(per_block)]
    my_returns = -functools.reduce(jnp.add, my_parts) - meta_all[c, 2:3, :]
    my_scores = jnp.broadcast_to((my_returns - mean) / scale, (8, rows))
    scores_ref[...] = lax.dot_general(my_scores, place_f, (((1,), (1,)), ((), ())),
                                      precision=HI, preferred_element_type=F32)[0:1]

    for cp in win_copies + act_copies + side_copies:
        cp.wait_send()

    @pl.when(owner)
    def _():
        for cp in ret_copies:
            cp.wait_send()


def on_device(n_cand, n_tp, start_state, goal, mean_prev, std_prev, noise, members, elites, w_in, w_hid, w_out):
    local = noise.shape[0]
    n_mem, depth, chunk = w_in.shape
    width = start_state.shape[0]
    flat = mean_prev.shape[0]
    hidden = w_hid.shape[1]
    cap = -(-(5 * local // 16) // 16) * 16
    rows = n_mem * cap
    n_own = n_tp - 2 * (n_tp // 4)
    own = rows // n_own
    total = n_cand * n_tp
    vmem = pl.BlockSpec(memory_space=pltpu.VMEM)
    hbm = pl.BlockSpec(memory_space=pl.ANY)
    dma = pltpu.SemaphoreType.DMA
    scores, new_mean, new_std = pl.pallas_call(
        functools.partial(kernel, n_cand, n_tp, cap),
        out_shape=(
            jax.ShapeDtypeStruct((1, local), F32),
            jax.ShapeDtypeStruct((1, flat), F32),
            jax.ShapeDtypeStruct((1, flat), F32),
        ),
        in_specs=[vmem] * 7 + [hbm] * 3,
        out_specs=(vmem,) * 3,
        scratch_shapes=[
            pltpu.VMEM((n_tp, depth, chunk), BF16),
            pltpu.VMEM((hidden, chunk), BF16),
            pltpu.VMEM((chunk, width), BF16),
            pltpu.VMEM((rows, hidden), BF16),
            pltpu.VMEM((rows, width), F32),
            pltpu.VMEM((rows, width), BF16),
            pltpu.VMEM((n_tp, own, width), BF16),
            pltpu.VMEM((rows, width), BF16),
            pltpu.VMEM((own, width), BF16),
            pltpu.VMEM((own, width), F32),
            pltpu.VMEM((own, width), F32),
            pltpu.VMEM((rows, width), F32),
            pltpu.VMEM((rows, flat), BF16),
            pltpu.VMEM((rows, flat), BF16),
            pltpu.VMEM((HORIZON, rows, flat // HORIZON), BF16),
            pltpu.VMEM((n_cand, rows, flat), F32),
            pltpu.VMEM((n_cand, 8, rows), F32),
            pltpu.VMEM((n_cand * n_own, 1, rows), F32),
            dma((3,)),
            dma((n_tp,)), dma((n_tp,)),
            dma((n_mem,)), dma((n_mem,)),
            dma((n_cand,)), dma((n_cand,)),
            dma((n_cand,)), dma((n_cand,)),
            dma((n_tp,)), dma((n_tp,)),
            dma((n_tp,)), dma((n_tp,)),
            dma((total,)), dma((total,)),
        ],
        compiler_params=pltpu.CompilerParams(has_side_effects=True, vmem_limit_bytes=56 << 20),
    )(
        start_state.reshape(1, -1), goal.reshape(1, -1), mean_prev.reshape(1, -1),
        std_prev.reshape(1, -1), noise, members, elites.reshape(1, -1), w_in, w_hid, w_out,
    )
    return scores.reshape(-1), new_mean.reshape(-1), new_std.reshape(-1)


def solution(mesh):
    placed = (
        P(), P(), P(), P(), P("cand", None), P("cand", None), P(),
        P(None, None, "tp"), P(None, None, "tp"), P(None, "tp", None),
    )
    return jax.shard_map(
        functools.partial(on_device, mesh.shape["cand"], mesh.shape["tp"]),
        mesh=mesh, in_specs=placed, out_specs=(P("cand"), P(), P()), check_vma=False,
    )
```
